32 devices in a mesh: row: 8 (over y, x, core), col: 4 (over z).
Axes of the slice: x: 2, y: 2, z: 4, core: 2. Of those that a mesh axis runs over, the one named last changes fastest.
Arguments:
- rotation: bfloat16 [8192, 8192], P('row', 'col'), may hold values from -0.0625 to 0.0625
- gradient: bfloat16 [8192, 8192], P('row', 'col'), may hold values from -0.0625 to 0.0625
Outputs:
- updated: float32 [8192, 2048], P('row', 'col')
- column_norms: float32 [2048], P('col')
The draws below stay inside these ranges and needn't reach their ends.
All inputs are finite; a program needn't handle non-finite values.
Results may differ from the reference program's by a relative error of at most 0.01.
Values may be sent and summed in bfloat16 or wider, within the bound.
A program may use at most 128 MiB of HBM per device.

```python
import jax
import jax.numpy as jnp
from jax import lax

N = 8192
SLAB = 2048
N_ROW = 8


def levels(key, dims, split, least, high):
    level = 1.0
    for axis_at, blocks in split:
        steps = jax.random.uniform(jax.random.fold_in(jax.random.fold_in(key, 6), axis_at), (blocks,), jnp.float32, least / len(split), high / len(split))
        level = level * jnp.repeat(jnp.exp(steps), dims[axis_at] // blocks).reshape((-1,) + (1,) * (len(dims) - 1 - axis_at))
    return level


def normal_values(own_key, extent, width, most, cuts=(), kind=jnp.bfloat16):
    values = width * jax.random.normal(own_key, extent, jnp.float32)
    if cuts:
        values = values * levels(own_key, extent, cuts, -0.22, 0.18)
    return jnp.clip(values, -most, most).astype(kind)


def setup_inputs(seed: int = 0) -> dict:
    seeds = jax.random.split(jax.random.key(seed), 3)
    return {
        "rotation": normal_values(seeds[0], (N, N), N ** -0.5, 0.0625, ((0, 8), (1, 4))),
        "gradient": normal_values(seeds[1], (N, N), N ** -0.5, 0.0625, ((0, 8), (1, 4))),
    }


def apply_generator(rotation, gradient, panel):
    block = N // N_ROW
    rot_blocks = rotation.reshape(N_ROW, block, N)
    grad_blocks = gradient.reshape(N_ROW, block, N)
    pan_blocks = panel.reshape(N_ROW, block, panel.shape[1])

    def add_block(carry, pieces):
        rot_piece, grad_piece, pan_piece = pieces
        left = jnp.dot(rot_piece.T, pan_piece, preferred_element_type=jnp.float32)
        right = jnp.dot(grad_piece.T, pan_piece, preferred_element_type=jnp.float32)
        left = lax.optimization_barrier(left.astype(jnp.bfloat16)).astype(jnp.float32)
        right = lax.optimization_barrier(right.astype(jnp.bfloat16)).astype(jnp.float32)
        return ((carry[0] + left, carry[1] + right), None)
    zeros = jnp.zeros((N, panel.shape[1]), jnp.float32)
    (left_sum, right_sum), _ = lax.scan(add_block, (zeros, zeros), (rot_blocks, grad_blocks, pan_blocks))
    left_sum = left_sum.astype(jnp.bfloat16)
    right_sum = right_sum.astype(jnp.bfloat16)
    return jnp.dot(gradient, left_sum, preferred_element_type=jnp.float32) - jnp.dot(rotation, right_sum, preferred_element_type=jnp.float32)

def reference(rotation, gradient):
    base = rotation[:, ::N // SLAB]
    base_wide = base.astype(jnp.float32)
    first = base_wide + 0.25 * apply_generator(rotation, gradient, base)
    middle = (base_wide + first).astype(jnp.bfloat16)
    updated = base_wide + 0.125 * apply_generator(rotation, gradient, middle)
    column_norms = jnp.sqrt(lax.optimization_barrier(jnp.sum(updated * updated, axis=0)))
    return (updated, column_norms)
```

```python
import functools

import jax
import jax.numpy as jnp
from jax import lax
from jax.sharding import PartitionSpec as P

N = 8192
SLAB = 2048
PIECES = 2


def wide(x):
    return x.astype(jnp.float32)


def swap(x, bit, n_row):
    return lax.ppermute(x, "row", [(i, i ^ bit) for i in range(n_row)])


def shift(x, step, n_col):
    return lax.ppermute(x, "col", [(i, (i + step) % n_col) for i in range(n_col)])


def gather_columns(x, step, n_col):
    slots = [x]
    for _ in range(n_col - 1):
        slots.append(shift(slots[-1], step, n_col))
    return jnp.concatenate(slots, axis=1)


def scatter_columns(term, step, n_col):
    width = term.shape[1] // n_col
    slots = [term[:, t * width : (t + 1) * width] for t in range(n_col)]
    if n_col == 1:
        return slots[0]
    total = slots[1].astype(jnp.bfloat16)
    for t in range(2, n_col):
        total = (wide(shift(total, step, n_col)) + slots[t]).astype(jnp.bfloat16)
    return wide(shift(total, step, n_col)) + slots[0]


def sum_over_chips(z, levels, order, n_row):
    depth, columns = z.shape
    z = z.reshape((2,) * levels + (depth >> levels, columns))
    left = list(range(levels - 1, -1, -1))
    places = []
    for b in order:
        place = left.index(b)
        left.remove(b)
        places.append(place)
        keep = lax.index_in_dim(z, 0, place, keepdims=False)
        send = lax.index_in_dim(z, 1, place, keepdims=False)
        z = (wide(keep) + wide(swap(send, 2 << b, n_row))).astype(jnp.bfloat16)
    for b, place in zip(reversed(order), reversed(places)):
        z = jnp.stack([z, swap(z, 2 << b, n_row)], axis=place)
    return z.reshape(depth, columns)


def on_device(n_row, n_col, rotation, gradient):
    stride = N // SLAB
    rows, width = rotation.shape
    own = width // stride // 2
    part = own // PIECES
    levels = n_row.bit_length() - 2
    blocks = 1 << levels
    block = width // blocks
    at = lax.axis_index("row")
    core, chip = at & 1, at >> 1

    def pair_rows(x):
        both = jnp.concatenate([x, swap(x, 1, n_row)], axis=0)
        return jnp.concatenate(
            [lax.dynamic_slice_in_dim(both, (q ^ chip) * block, block, axis=1) for q in range(blocks)],
            axis=1,
        )

    rot = pair_rows(rotation)
    grad = pair_rows(gradient)

    k = lax.broadcasted_iota(jnp.int32, (width, own), 0)
    j = lax.broadcasted_iota(jnp.int32, (width, own), 1)
    column = ((k // block) ^ chip) * block + k % block
    pick = (column == stride * (core * own + j)).astype(jnp.bfloat16)
    base = jnp.dot(rot, pick, preferred_element_type=jnp.float32).astype(jnp.bfloat16)

    up, down = tuple(range(levels)), tuple(range(levels - 1, -1, -1))

    def apply_generator(panel, step):
        v = gather_columns(panel, step, n_col)
        z1 = jnp.einsum("ik,is->ks", rot, v, preferred_element_type=jnp.float32).astype(jnp.bfloat16)
        z2 = jnp.einsum("ik,is->ks", grad, v, preferred_element_type=jnp.float32).astype(jnp.bfloat16)
        z1 = sum_over_chips(z1, levels, up, n_row)
        z2 = sum_over_chips(z2, levels, down, n_row)
        term = jnp.dot(grad, z1, preferred_element_type=jnp.float32) - jnp.dot(
            rot, z2, preferred_element_type=jnp.float32
        )
        return scatter_columns(term, step, n_col)

    mine, other, squares = [], [], []
    for p in range(PIECES):
        step = 1 if p % 2 == 0 else -1
        panel = base[:, p * part : (p + 1) * part]
        first = wide(panel) + 0.25 * apply_generator(panel, step)
        middle = (wide(panel) + first).astype(jnp.bfloat16)
        updated = wide(panel) + 0.125 * apply_generator(middle, step)
        mine.append(updated[:rows])
        other.append(swap(updated[rows:], 1, n_row))
        squares.append(jnp.sum(updated * updated, axis=0))

    def in_order(a, b):
        return jnp.where(core == 0, jnp.concatenate([a, b], axis=-1), jnp.concatenate([b, a], axis=-1))

    updated = in_order(jnp.concatenate(mine, axis=1), jnp.concatenate(other, axis=1))
    total = jnp.concatenate(squares)
    for b in range(levels):
        total = total + swap(total, 2 << b, n_row)
    return updated, jnp.sqrt(in_order(total, swap(total, 1, n_row)))


def solution(mesh):
    placed = (P("row", "col"), P("row", "col"))
    return jax.shard_map(
        functools.partial(on_device, mesh.shape["row"], mesh.shape["col"]),
        mesh=mesh,
        in_specs=placed,
        out_specs=(P("row", "col"), P("col")),
        check_vma=False,
    )
```
